32 devices in a mesh: clip: 2 (over y), outer: 4 (over z), inner: 2 (over x), head: 2 (over core).
Axes of the slice: x: 2, y: 2, z: 4, core: 2. Of those that a mesh axis runs over, the one named last changes fastest.
Arguments:
- tokens: bfloat16 [2, 4096, 3072], P('clip', ('outer', 'inner', 'head')), parts along dimension 0, may hold values from -6 to 6
- shift_mod: float32 [2, 3072], P('clip'), parts along dimension 0, may hold values from -3 to 3
- scale_mod: float32 [2, 3072], P('clip'), parts along dimension 0, may hold values from -1.5 to 1.5
- gate_mod: float32 [2, 3072], P('clip'), parts along dimension 0, may hold values from 0.5 to 2
- query_weight: bfloat16 [3072, 3072], P('outer', ('inner', 'head')), may hold values from -0.109375 to 0.109375
- key_weight: bfloat16 [3072, 3072], P('outer', ('inner', 'head')), may hold values from -0.109375 to 0.109375
- value_weight: bfloat16 [3072, 3072], P('outer', ('inner', 'head')), may hold values from -0.109375 to 0.109375
- out_weight: bfloat16 [3072, 3072], P(('inner', 'head'), 'outer'), may hold values from -0.109375 to 0.109375
- query_gain: float32 [128], replicated, may hold values from 1 to 18, as said below
- key_gain: float32 [128], replicated, may hold values from 1 to 18, as said below
Outputs:
- attended: bfloat16 [2, 4096, 3072], P('clip', ('outer', 'inner', 'head')), parts along dimension 0
The draws below stay inside these ranges and needn't reach their ends.
There are 2 independent parts, one for each index of `clip`. The reference program is written for one: setup_inputs(seed, part) draws one part's arguments, and reference() takes and returns one part's arrays. A program takes and returns all parts, laid end to end along the dimension named above; an argument that names none is the same for every part. Nothing has to cross between parts.
Inputs may be any that keep to these rules, and one draw needn't show every extreme that they name: `query_gain`: 128 positive scales. `key_gain`: 128 positive scales.
All inputs are finite; a program needn't handle non-finite values.
Results may differ from the reference program's by a relative error of at most 0.015.
The reference program's roundings to bfloat16 on the way (of `modulated`, `value_heads`, `mixed` and `group_term`) count: a program that leaves them out, or rounds other values in their place, can miss the bound.
Values may be sent and summed in bfloat16 or wider, within the bound.
A program may use at most 192 MiB of HBM per device.

```python
import math
import jax
import jax.numpy as jnp
from jax import lax

D = 3072
HEADS = 24
HD = 128
S = 4096
CLIPS = 1
N_INNER = 2
N_HEAD = 2


def base_gain(key):
    lower_log = jnp.log(jnp.float32(1.0))
    upper_log = jnp.log(jnp.float32(2.0))
    return jnp.exp(jax.random.uniform(key, (HD,), jnp.float32, lower_log, upper_log))


def draw_query_gain(key, part):
    gain_values = base_gain(jax.random.fold_in(key, 1))
    return gain_values


def draw_key_gain(key, part):
    gain_values = base_gain(jax.random.fold_in(key, 2))
    return gain_values


def levels(stream_key, dims, cuts, least, high):
    factor_of = 1.0
    for position, shards_of in cuts:
        steps = jax.random.uniform(jax.random.fold_in(jax.random.fold_in(stream_key, 6), position), (shards_of,), jnp.float32, least / len(cuts), high / len(cuts))
        factor_of = factor_of * jnp.repeat(jnp.exp(steps), dims[position] // shards_of).reshape((-1,) + (1,) * (len(dims) - 1 - position))
    return factor_of


def noise(rng, dims, scale, limit, shards=(), held_as=jnp.bfloat16):
    entries = jax.random.normal(rng, dims, jnp.float32) * scale
    if len(shards) > 0:
        entries = levels(rng, dims, shards, -0.22, 0.18) * entries
    return jnp.clip(entries, min=-limit, max=limit).astype(held_as)


def setup_inputs(seed: int = 0, part: int = 0) -> dict:
    keys = jax.random.split(jax.random.key(seed), 11)
    own_keys = jax.random.split(jax.random.fold_in(keys[10], part), 11)
    return {
        "tokens": noise(own_keys[0], (CLIPS, S, D), 1.0, 6.0, ((1, 16),)),
        "shift_mod": noise(own_keys[1], (CLIPS, D), 0.5, 3.0, (), jnp.float32),
        "scale_mod": noise(own_keys[2], (CLIPS, D), 0.3, 1.5, (), jnp.float32),
        "gate_mod": jnp.clip(jax.random.uniform(own_keys[3], (CLIPS, D), jnp.float32, 0.5, 2.0), 0.5, 2.0),
        "query_weight": noise(keys[4], (D, HEADS * HD), D ** -0.5, 0.109375, ((0, 4), (1, 4))),
        "key_weight": noise(keys[5], (D, HEADS * HD), D ** -0.5, 0.109375, ((0, 4), (1, 4))),
        "value_weight": noise(keys[6], (D, HEADS * HD), D ** -0.5, 0.109375, ((0, 4), (1, 4))),
        "out_weight": noise(keys[7], (HEADS * HD, D), (HEADS * HD) ** -0.5, 0.109375, ((0, 4), (1, 4))),
        "query_gain": draw_query_gain(jax.random.fold_in(keys[10], 71), part),
        "key_gain": draw_key_gain(jax.random.fold_in(keys[10], 71), part),
    }


EPSILON = 1e-06

def modulate(tokens, shift_mod, scale_mod):
    values = tokens.astype(jnp.float32)
    center = lax.optimization_barrier(jnp.mean(values, axis=-1, keepdims=True))
    spread = lax.optimization_barrier(jnp.mean(jnp.square(values - center), axis=-1, keepdims=True))
    normed = (values - center) / jnp.sqrt(spread + EPSILON)
    return (normed * (1.0 + scale_mod[:, None, :]) + shift_mod[:, None, :]).astype(jnp.bfloat16)

def head_norm(projected, gain_vec, head_dim):
    shaped = projected.reshape(projected.shape[:-1] + (projected.shape[-1] // head_dim, head_dim))
    mean_square = lax.optimization_barrier(jnp.mean(jnp.square(shaped), axis=-1, keepdims=True))
    return (shaped / jnp.sqrt(mean_square + EPSILON) * gain_vec).astype(jnp.bfloat16)

def one_head(operands):
    query_one, key_one, value_one = operands
    scores = jnp.einsum('cqd,ckd->cqk', query_one.astype(jnp.float32), key_one.astype(jnp.float32), precision=lax.Precision.HIGHEST) / math.sqrt(HD)
    row_max = lax.optimization_barrier(jnp.max(scores, axis=-1, keepdims=True))
    weights = jnp.exp(scores - row_max)
    row_total = lax.optimization_barrier(jnp.sum(weights, axis=-1, keepdims=True))
    rounded = lax.optimization_barrier(weights.astype(jnp.bfloat16))
    mixed_values = jnp.einsum('cqk,ckd->cqd', rounded.astype(jnp.float32), value_one.astype(jnp.float32), precision=lax.Precision.HIGHEST)
    return mixed_values / row_total

def reference(tokens, shift_mod, scale_mod, gate_mod, query_weight, key_weight, value_weight, out_weight, query_gain, key_gain):
    clip_count = tokens.shape[0]
    all_cols = HEADS * HD
    modulated = modulate(tokens, shift_mod, scale_mod).reshape(clip_count * S, D)
    query_proj = jnp.dot(modulated, query_weight, preferred_element_type=jnp.float32)
    key_proj = jnp.dot(modulated, key_weight, preferred_element_type=jnp.float32)
    value_proj = jnp.dot(modulated, value_weight, preferred_element_type=jnp.float32)
    query_heads = lax.optimization_barrier(head_norm(query_proj.reshape(clip_count, S, all_cols), query_gain, HD))
    key_heads = lax.optimization_barrier(head_norm(key_proj.reshape(clip_count, S, all_cols), key_gain, HD))
    value_heads = lax.optimization_barrier(value_proj.astype(jnp.bfloat16).reshape(clip_count, S, HEADS, HD))
    stacked = (jnp.transpose(query_heads, (2, 0, 1, 3)), jnp.transpose(key_heads, (2, 0, 1, 3)), jnp.transpose(value_heads, (2, 0, 1, 3)))
    head_out = lax.map(one_head, stacked)
    mixed = jnp.transpose(head_out, (1, 2, 0, 3)).reshape(clip_count * S, all_cols).astype(jnp.bfloat16)
    groups = N_INNER * N_HEAD
    group_width = all_cols // groups
    summed = jnp.zeros((clip_count * S, D), jnp.float32)
    for group_index in range(groups):
        lower = group_index * group_width
        group_term = jnp.dot(mixed[:, lower:lower + group_width], out_weight[lower:lower + group_width, :], preferred_element_type=jnp.float32).astype(jnp.bfloat16)
        group_term = lax.optimization_barrier(group_term)
        summed = summed + group_term.astype(jnp.float32)
    return (summed.reshape(clip_count, S, D) * gate_mod[:, None, :]).astype(jnp.bfloat16)
```

```python
import functools
import math

import jax
import jax.numpy as jnp
from jax import lax
from jax.experimental import pallas as pl
from jax.experimental.pallas import tpu as pltpu
from jax.sharding import PartitionSpec as P

EPSILON = 1e-06


def modulate(tokens, shift_mod, scale_mod):
    values = tokens.astype(jnp.float32)
    center = jnp.mean(values, axis=-1, keepdims=True)
    spread = jnp.mean(jnp.square(values - center), axis=-1, keepdims=True)
    normed = (values - center) / jnp.sqrt(spread + EPSILON)
    return (normed * (1.0 + scale_mod[:, None, :]) + shift_mod[:, None, :]).astype(jnp.bfloat16)


def head_norm(projected, gain_vec, head_dim):
    shaped = projected.reshape(projected.shape[:-1] + (projected.shape[-1] // head_dim, head_dim))
    mean_square = jnp.mean(jnp.square(shaped), axis=-1, keepdims=True)
    return (shaped / jnp.sqrt(mean_square + EPSILON) * gain_vec).astype(jnp.bfloat16)


def per_device(
    tokens,
    shift_mod,
    scale_mod,
    gate_mod,
    query_weight,
    key_weight,
    value_weight,
    out_weight,
    query_gain,
    key_gain,
):
    head_dim = query_gain.shape[0]
    modulated = modulate(tokens, shift_mod, scale_mod)
    gathered = lax.all_gather(modulated, ("inner", "head"), axis=1, tiled=True)
    clip_count, row_count, model_width = gathered.shape
    flattened = gathered.reshape(clip_count * row_count, model_width)
    local_cols = query_weight.shape[1]
    head_count = local_cols // head_dim
    full_query, full_key, full_value = (
        lax.all_gather(query_weight, "outer", axis=0, tiled=True),
        lax.all_gather(key_weight, "outer", axis=0, tiled=True),
        lax.all_gather(value_weight, "outer", axis=0, tiled=True),
    )
    query_proj = jnp.dot(flattened, full_query, preferred_element_type=jnp.float32)
    key_proj = jnp.dot(flattened, full_key, preferred_element_type=jnp.float32)
    value_proj = jnp.dot(flattened, full_value, preferred_element_type=jnp.float32)
    query_heads = head_norm(
        query_proj.reshape(clip_count, row_count, local_cols), query_gain, head_dim
    )
    key_send = head_norm(key_proj.reshape(clip_count, row_count, local_cols), key_gain, head_dim)
    key_send = key_send.reshape(clip_count, row_count, local_cols)
    value_send = value_proj.astype(jnp.bfloat16).reshape(clip_count, row_count, local_cols)
    root_size = math.sqrt(head_dim)
    full_out = lax.all_gather(out_weight, "outer", axis=1, tiled=True)
    running_max = jnp.full((clip_count, head_count, row_count), -1e30, jnp.float32)
    key_piece = lax.all_gather(key_send, "outer", axis=1, tiled=True)
    value_piece = lax.all_gather(value_send, "outer", axis=1, tiled=True)
    key_count = key_piece.shape[1]
    key_piece = key_piece.reshape(clip_count, key_count, head_count, head_dim)
    value_piece = value_piece.reshape(clip_count, key_count, head_count, head_dim)
    scores = (
        jnp.einsum("cqhd,ckhd->chqk", query_heads, key_piece, preferred_element_type=jnp.float32)
        / root_size
    )
    new_max = jnp.maximum(running_max, jnp.max(scores, axis=-1))
    weights = jnp.exp(scores - new_max[..., None])
    new_sum = jnp.sum(weights, axis=-1)
    new_acc = jnp.einsum(
        "chqk,ckhd->chqd",
        weights.astype(jnp.bfloat16),
        value_piece,
        preferred_element_type=jnp.float32,
    )
    head_out = new_acc / new_sum[..., None]
    mixed = (
        jnp.transpose(head_out, (0, 2, 1, 3))
        .reshape(clip_count * row_count, local_cols)
        .astype(jnp.bfloat16)
    )
    partial_value = jnp.dot(mixed, full_out, preferred_element_type=jnp.float32).reshape(
        clip_count, row_count, -1
    )
    summed = lax.psum_scatter(
        partial_value.astype(jnp.bfloat16), ("inner", "head"), scatter_dimension=1, tiled=True
    ).astype(jnp.float32)
    return (summed * gate_mod[:, None, :]).astype(jnp.bfloat16)


def attend_tile(scale, query_ref, key_ref, value_ref, out_ref):
    scores = lax.dot_general(
        query_ref[...], key_ref[...], (((1,), (1,)), ((), ())), preferred_element_type=jnp.float32
    )
    row_max = jnp.max(scores, axis=-1, keepdims=True)
    weights = jnp.exp2((scores - row_max) * scale)
    total = jnp.sum(weights, axis=-1, keepdims=True)
    mixed = jnp.dot(
        weights.astype(jnp.bfloat16), value_ref[...], preferred_element_type=jnp.float32
    )
    out_ref[...] = (mixed / total).astype(jnp.bfloat16)


def attend(query, key, value, tile=256):
    rows, head_dim = query.shape
    keys = key.shape[0]
    while rows % tile:
        tile //= 2
    return pl.pallas_call(
        functools.partial(attend_tile, math.log2(math.e) / math.sqrt(head_dim)),
        out_shape=jax.ShapeDtypeStruct((rows, head_dim), jnp.bfloat16),
        grid=(rows // tile,),
        in_specs=[
            pl.BlockSpec((tile, head_dim), lambda i: (i, 0)),
            pl.BlockSpec((keys, head_dim), lambda i: (0, 0)),
            pl.BlockSpec((keys, head_dim), lambda i: (0, 0)),
        ],
        out_specs=pl.BlockSpec((tile, head_dim), lambda i: (i, 0)),
        compiler_params=pltpu.CompilerParams(vmem_limit_bytes=56 * 1024 * 1024),
        cost_estimate=pl.CostEstimate(
            flops=8 * rows * keys * head_dim,
            bytes_accessed=4 * (rows + keys) * head_dim,
            transcendentals=rows * keys,
        ),
        name="attend",
    )(query, key, value)


def norm_columns(projected, gain_vec):
    mean_square = jnp.mean(jnp.square(projected), axis=-1, keepdims=True)
    return (projected / jnp.sqrt(mean_square + EPSILON) * gain_vec).astype(jnp.bfloat16)


def after(value, *others):
    return lax.optimization_barrier((value,) + others)[0]


def swap(value, axis):
    return lax.ppermute(value, axis, [(0, 1), (1, 0)])


def head_sharded(
    clips,
    outers,
    tokens,
    shift_mod,
    scale_mod,
    gate_mod,
    query_weight,
    key_weight,
    value_weight,
    out_weight,
    query_gain,
    key_gain,
):
    head_dim = query_gain.shape[0]
    depth, local_cols = query_weight.shape
    spare = local_cols // head_dim > outers
    me = lax.axis_index("outer")
    clip = lax.axis_index("clip")
    hops = [1, outers - 1] + list(range(2, outers - 1))

    def send(value, hop):
        return lax.ppermute(value, "outer", [(i, (i + hop) % outers) for i in range(outers)])

    def back(value, hop):
        return lax.ppermute(value, "outer", [(i, (i - hop) % outers) for i in range(outers)])

    def columns(weight, head):
        return lax.dynamic_slice_in_dim(weight, head * head_dim, head_dim, axis=1)

    def weights_for(owner, rows=None):
        take = (lambda w: w) if rows is None else (
            lambda w: lax.dynamic_slice_in_dim(w, clip * rows, rows, axis=0)
        )
        wq, wk, wv = take(query_weight), take(key_weight), take(value_weight)
        if not spare:
            return jnp.concatenate([columns(w, owner) for w in (wq, wk, wv)], axis=1)
        extra = outers + owner // 2
        return jnp.concatenate(
            [columns(wq, owner)]
            + [columns(w, h) for w in (wk, wv) for h in (owner, extra)]
            + [columns(wq, extra)],
            axis=1,
        )

    part = depth // clips
    arrived = [send(weights_for((me + hop) % outers, part), hop) for hop in hops]
    modulated = modulate(tokens, shift_mod, scale_mod)[0]
    own = weights_for(me)
    width = own.shape[1]
    full = jnp.zeros((outers * depth, width), jnp.bfloat16)
    full = lax.dynamic_update_slice(full, own, (me * depth, 0))
    for hop, piece in zip(hops, arrived):
        source = (me - hop) % outers
        full = lax.dynamic_update_slice(full, piece, (source * depth + clip * part, 0))
        if clips > 1:
            other = swap(piece, "clip")
            full = lax.dynamic_update_slice(
                full, other, (source * depth + (1 - clip) * part, 0)
            )

    def spread(piece):
        across = swap(piece, "inner")
        return jnp.concatenate(
            [piece, swap(piece, "head"), across, swap(across, "head")], axis=0
        )

    pieces = {0: modulated}
    gate_on = arrived
    for hop in hops:
        pieces[hop] = send(after(modulated, *gate_on), hop)
        gate_on = [pieces[hop]]

    out_full = jnp.zeros((local_cols, outers * out_weight.shape[1]), jnp.bfloat16)
    out_cols = out_weight.shape[1]
    out_full = lax.dynamic_update_slice(out_full, out_weight, (0, me * out_cols))
    out_part = local_cols // clips
    out_half = lax.dynamic_slice_in_dim(out_weight, clip * out_part, out_part, axis=0)
    out_half = after(out_half, *gate_on)
    for hop in hops:
        piece = send(out_half, hop)
        source = (me - hop) % outers
        out_full = lax.dynamic_update_slice(
            out_full, piece, (clip * out_part, source * out_cols)
        )
        if clips > 1:
            out_full = lax.dynamic_update_slice(
                out_full, swap(piece, "clip"), ((1 - clip) * out_part, source * out_cols)
            )

    queries, extra_queries = {}, {}
    keys, values = [[], []], [[], []]
    kv_heads = 2 if spare else 1
    for hop in [0] + hops:
        block = spread(pieces[hop])
        need_extra = spare and hop % 2 == 0
        weight = full if need_extra or not spare else full[:, : width - head_dim]
        projected = jnp.dot(block, weight, preferred_element_type=jnp.float32)
        cut = [projected[:, i : i + head_dim] for i in range(0, projected.shape[1], head_dim)]
        queries[hop] = norm_columns(cut[0], query_gain)
        for h in range(kv_heads):
            keys[h].append(norm_columns(cut[1 + h], key_gain))
            values[h].append(cut[1 + kv_heads + h].astype(jnp.bfloat16))
        if need_extra:
            extra_queries[hop] = norm_columns(cut[-1], query_gain)
    keys = [jnp.concatenate(k, axis=0) for k in keys[:kv_heads]]
    values = [jnp.concatenate(v, axis=0) for v in values[:kv_heads]]

    got, got_extra = {}, {}
    previous = None
    for hop in hops[::-1] + [0]:
        query = queries[hop] if previous is None else after(queries[hop], previous)
        result = attend(query, keys[0], values[0])
        if hop in extra_queries:
            extra_result = attend(after(extra_queries[hop], result), keys[1], values[1])
            got_extra[hop] = back(extra_result, hop) if hop else extra_result
            previous = extra_result
        else:
            previous = result
        got[hop] = back(result, hop) if hop else result

    stacked = jnp.stack([got[s] for s in range(outers)])
    heads = [
        lax.dynamic_index_in_dim(stacked, (h - me) % outers, axis=0, keepdims=False)
        for h in range(outers)
    ]
    if spare:
        evens = list(range(0, outers, 2))
        stacked_extra = jnp.stack([got_extra[s] for s in evens])
        for j in range(outers // 2):
            sender = 2 * j + me % 2
            heads.append(
                lax.dynamic_index_in_dim(
                    stacked_extra, ((sender - me) % outers) // 2, axis=0, keepdims=False
                )
            )
    mixed = jnp.concatenate(heads, axis=1)

    rows = tokens.shape[1]
    chunks = 2
    step = out_full.shape[1] // chunks
    outs = []
    far = []
    for c in range(chunks):
        cols = out_full[:, c * step : (c + 1) * step]
        far_terms = jnp.dot(
            mixed[2 * rows :], cols, preferred_element_type=jnp.float32
        ).astype(jnp.bfloat16)
        across = swap(far_terms[rows:], "head")
        both = (far_terms[:rows].astype(jnp.float32) + across.astype(jnp.float32)).astype(
            jnp.bfloat16
        )
        far.append(swap(both, "inner"))
    for c in range(chunks):
        cols = out_full[:, c * step : (c + 1) * step]
        near_terms = jnp.dot(
            mixed[: 2 * rows], cols, preferred_element_type=jnp.float32
        ).astype(jnp.bfloat16)
        near = swap(near_terms[rows:], "head")
        summed = (
            near_terms[:rows].astype(jnp.float32)
            + near.astype(jnp.float32)
            + far[c].astype(jnp.float32)
        )
        outs.append((summed * gate_mod[:, c * step : (c + 1) * step]).astype(jnp.bfloat16))
    return jnp.concatenate(outs, axis=1)[None]


def fits(mesh):
    sizes = mesh.shape
    return (
        sizes["inner"] == 2 and sizes["head"] == 2 and sizes["clip"] <= 2
        and 4 <= sizes["outer"] <= 8 and sizes["outer"] % 2 == 0
    )


def solution(mesh):
    in_specs = (
        P("clip", ("outer", "inner", "head"), None),
        P("clip", None),
        P("clip", None),
        P("clip", None),
        P("outer", ("inner", "head")),
        P("outer", ("inner", "head")),
        P("outer", ("inner", "head")),
        P(("inner", "head"), "outer"),
        P(),
        P(),
    )
    out_specs = P("clip", ("outer", "inner", "head"), None)

    def body(*args):
        clips, outers = mesh.shape["clip"], mesh.shape["outer"]
        head_count = args[4].shape[1] // args[8].shape[0]
        placed = 2 * head_count in (2 * outers, 3 * outers)
        if fits(mesh) and placed and args[0].shape[0] == 1:
            return head_sharded(clips, outers, *args)
        return per_device(*args)

    return jax.shard_map(
        body, mesh=mesh, in_specs=in_specs, out_specs=out_specs, check_vma=False
    )
```

```python
import functools
import math

import jax
import jax.numpy as jnp
from jax import lax
from jax.experimental import pallas as pl
from jax.experimental.pallas import tpu as pltpu
from jax.sharding import PartitionSpec as P

EPSILON = 1e-06


def modulate(tokens, shift_mod, scale_mod):
    values = tokens.astype(jnp.float32)
    center = jnp.mean(values, axis=-1, keepdims=True)
    spread = jnp.mean(jnp.square(values - center), axis=-1, keepdims=True)
    normed = (values - center) / jnp.sqrt(spread + EPSILON)
    return (normed * (1.0 + scale_mod[:, None, :]) + shift_mod[:, None, :]).astype(jnp.bfloat16)


def head_norm(projected, gain_vec, head_dim):
    shaped = projected.reshape(projected.shape[:-1] + (projected.shape[-1] // head_dim, head_dim))
    mean_square = jnp.mean(jnp.square(shaped), axis=-1, keepdims=True)
    return (shaped / jnp.sqrt(mean_square + EPSILON) * gain_vec).astype(jnp.bfloat16)


def per_device(
    tokens,
    shift_mod,
    scale_mod,
    gate_mod,
    query_weight,
    key_weight,
    value_weight,
    out_weight,
    query_gain,
    key_gain,
):
    head_dim = query_gain.shape[0]
    modulated = modulate(tokens, shift_mod, scale_mod)
    gathered = lax.all_gather(modulated, ("inner", "head"), axis=1, tiled=True)
    clip_count, row_count, model_width = gathered.shape
    flattened = gathered.reshape(clip_count * row_count, model_width)
    local_cols = query_weight.shape[1]
    head_count = local_cols // head_dim
    full_query, full_key, full_value = (
        lax.all_gather(query_weight, "outer", axis=0, tiled=True),
        lax.all_gather(key_weight, "outer", axis=0, tiled=True),
        lax.all_gather(value_weight, "outer", axis=0, tiled=True),
    )
    query_proj = jnp.dot(flattened, full_query, preferred_element_type=jnp.float32)
    key_proj = jnp.dot(flattened, full_key, preferred_element_type=jnp.float32)
    value_proj = jnp.dot(flattened, full_value, preferred_element_type=jnp.float32)
    query_heads = head_norm(
        query_proj.reshape(clip_count, row_count, local_cols), query_gain, head_dim
    )
    key_send = head_norm(key_proj.reshape(clip_count, row_count, local_cols), key_gain, head_dim)
    key_send = key_send.reshape(clip_count, row_count, local_cols)
    value_send = value_proj.astype(jnp.bfloat16).reshape(clip_count, row_count, local_cols)
    root_size = math.sqrt(head_dim)
    full_out = lax.all_gather(out_weight, "outer", axis=1, tiled=True)
    running_max = jnp.full((clip_count, head_count, row_count), -1e30, jnp.float32)
    key_piece = lax.all_gather(key_send, "outer", axis=1, tiled=True)
    value_piece = lax.all_gather(value_send, "outer", axis=1, tiled=True)
    key_count = key_piece.shape[1]
    key_piece = key_piece.reshape(clip_count, key_count, head_count, head_dim)
    value_piece = value_piece.reshape(clip_count, key_count, head_count, head_dim)
    scores = (
        jnp.einsum("cqhd,ckhd->chqk", query_heads, key_piece, preferred_element_type=jnp.float32)
        / root_size
    )
    new_max = jnp.maximum(running_max, jnp.max(scores, axis=-1))
    weights = jnp.exp(scores - new_max[..., None])
    new_sum = jnp.sum(weights, axis=-1)
    new_acc = jnp.einsum(
        "chqk,ckhd->chqd",
        weights.astype(jnp.bfloat16),
        value_piece,
        preferred_element_type=jnp.float32,
    )
    head_out = new_acc / new_sum[..., None]
    mixed = (
        jnp.transpose(head_out, (0, 2, 1, 3))
        .reshape(clip_count * row_count, local_cols)
        .astype(jnp.bfloat16)
    )
    partial_value = jnp.dot(mixed, full_out, preferred_element_type=jnp.float32).reshape(
        clip_count, row_count, -1
    )
    summed = lax.psum_scatter(
        partial_value.astype(jnp.bfloat16), ("inner", "head"), scatter_dimension=1, tiled=True
    ).astype(jnp.float32)
    return (summed * gate_mod[:, None, :]).astype(jnp.bfloat16)


def attend_tile(scale, query_ref, key_ref, value_ref, out_ref):
    scores = lax.dot_general(
        query_ref[...], key_ref[0], (((1,), (1,)), ((), ())), preferred_element_type=jnp.float32
    )
    row_max = jnp.max(scores, axis=-1, keepdims=True)
    weights = jnp.exp2((scores - row_max) * scale)
    total = jnp.sum(weights, axis=-1, keepdims=True)
    mixed = jnp.dot(
        weights.astype(jnp.bfloat16), value_ref[0], preferred_element_type=jnp.float32
    )
    out_ref[...] = (mixed / total).astype(jnp.bfloat16)


def attend(query, first_rows, key, value, tile=256):
    rows, head_dim = query.shape
    keys = key.shape[1]
    while rows % tile or first_rows % tile:
        tile //= 2
    edge = first_rows // tile
    return pl.pallas_call(
        functools.partial(attend_tile, math.log2(math.e) / math.sqrt(head_dim)),
        out_shape=jax.ShapeDtypeStruct((rows, head_dim), jnp.bfloat16),
        grid=(rows // tile,),
        in_specs=[
            pl.BlockSpec((tile, head_dim), lambda i: (i, 0)),
            pl.BlockSpec((1, keys, head_dim), lambda i: (jnp.where(i < edge, 0, 1), 0, 0)),
            pl.BlockSpec((1, keys, head_dim), lambda i: (jnp.where(i < edge, 0, 1), 0, 0)),
        ],
        out_specs=pl.BlockSpec((tile, head_dim), lambda i: (i, 0)),
        compiler_params=pltpu.CompilerParams(vmem_limit_bytes=56 * 1024 * 1024),
        cost_estimate=pl.CostEstimate(
            flops=8 * rows * keys * head_dim,
            bytes_accessed=4 * (rows + keys) * head_dim,
            transcendentals=rows * keys,
        ),
        name="attend",
    )(query, key, value)


def norm_columns(projected, gain_vec):
    mean_square = jnp.mean(jnp.square(projected), axis=-1, keepdims=True)
    return (projected / jnp.sqrt(mean_square + EPSILON) * gain_vec).astype(jnp.bfloat16)


def after(value, *others):
    return lax.optimization_barrier((value,) + others)[0]


def swap(value, axis):
    return lax.ppermute(value, axis, [(0, 1), (1, 0)])


def head_sharded(
    clips,
    outers,
    tokens,
    shift_mod,
    scale_mod,
    gate_mod,
    query_weight,
    key_weight,
    value_weight,
    out_weight,
    query_gain,
    key_gain,
):
    head_dim = query_gain.shape[0]
    depth, local_cols = query_weight.shape
    spare = local_cols // head_dim > outers
    me = lax.axis_index("outer")
    clip = lax.axis_index("clip")
    hops = [1, outers - 1] + list(range(2, outers - 1))

    def send(value, hop):
        return lax.ppermute(value, "outer", [(i, (i + hop) % outers) for i in range(outers)])

    def back(value, hop):
        return lax.ppermute(value, "outer", [(i, (i - hop) % outers) for i in range(outers)])

    def columns(weight, head):
        return lax.dynamic_slice_in_dim(weight, head * head_dim, head_dim, axis=1)

    def weights_for(owner, rows=None):
        take = (lambda w: w) if rows is None else (
            lambda w: lax.dynamic_slice_in_dim(w, clip * rows, rows, axis=0)
        )
        wq, wk, wv = take(query_weight), take(key_weight), take(value_weight)
        if not spare:
            return jnp.concatenate([columns(w, owner) for w in (wq, wk, wv)], axis=1)
        extra = outers + owner // 2
        return jnp.concatenate(
            [columns(wq, owner)]
            + [columns(w, h) for w in (wk, wv) for h in (owner, extra)]
            + [columns(wq, extra)],
            axis=1,
        )

    part = depth // clips
    arrived = [send(weights_for((me + hop) % outers, part), hop) for hop in hops]
    modulated = modulate(tokens, shift_mod, scale_mod)[0]
    own = weights_for(me)
    width = own.shape[1]
    full = jnp.zeros((outers * depth, width), jnp.bfloat16)
    full = lax.dynamic_update_slice(full, own, (me * depth, 0))
    for hop, piece in zip(hops, arrived):
        source = (me - hop) % outers
        full = lax.dynamic_update_slice(full, piece, (source * depth + clip * part, 0))
        if clips > 1:
            other = swap(piece, "clip")
            full = lax.dynamic_update_slice(
                full, other, (source * depth + (1 - clip) * part, 0)
            )

    def spread(piece):
        across = swap(piece, "inner")
        return jnp.concatenate(
            [piece, swap(piece, "head"), across, swap(across, "head")], axis=0
        )

    half = modulated.shape[0] // 2
    pieces = {0: (modulated[:half], modulated[half:])}
    ready = after(modulated, *arrived)
    moving = (ready[:half], ready[half:])
    for hop in range(1, outers):
        moving = tuple(send(piece, 1) for piece in moving)
        pieces[hop] = moving

    queries, extra_queries = {}, {}
    keys, values = [[], []], [[], []]
    kv_heads = 2 if spare else 1
    projected = None
    for hop in range(outers):
        need_extra = spare and hop % 2 == 0
        weight = full if need_extra or not spare else full[:, : width - head_dim]
        queries[hop], extra_queries[hop] = [], []
        for piece in pieces[hop]:
            projected = jnp.dot(spread(piece), weight, preferred_element_type=jnp.float32)
            cut = [projected[:, i : i + head_dim] for i in range(0, projected.shape[1], head_dim)]
            queries[hop].append(norm_columns(cut[0], query_gain))
            for h in range(kv_heads):
                keys[h].append(norm_columns(cut[1 + h], key_gain))
                values[h].append(cut[1 + kv_heads + h].astype(jnp.bfloat16))
            if need_extra:
                extra_queries[hop].append(norm_columns(cut[-1], query_gain))
    keys = jnp.stack([jnp.concatenate(k, axis=0) for k in keys[:kv_heads]])
    values = jnp.stack([jnp.concatenate(v, axis=0) for v in values[:kv_heads]])

    out_part = local_cols // clips
    out_full = jnp.zeros((outers,) + out_weight.shape, jnp.bfloat16)
    out_full = lax.dynamic_update_slice(out_full, out_weight[None], (me, 0, 0))
    moving_out = after(
        lax.dynamic_slice_in_dim(out_weight, clip * out_part, out_part, axis=0), *moving
    )
    for hop in range(1, outers):
        moving_out = send(moving_out, 1)
        source = (me - hop) % outers
        landed = after(moving_out, projected)
        out_full = lax.dynamic_update_slice(
            out_full, landed[None], (source, clip * out_part, 0)
        )
        if clips > 1:
            out_full = lax.dynamic_update_slice(
                out_full, swap(landed, "clip")[None], (source, (1 - clip) * out_part, 0)
            )

    def attended_heads(far, gate):
        def rows_of(parts):
            middle = parts[0].shape[0] // 2
            return [p[middle:] if far else p[:middle] for p in parts]

        def pick(hops):
            first = [p for s in hops for p in rows_of(queries[s])]
            second = [p for s in hops if extra_queries[s] for p in rows_of(extra_queries[s])]
            count = sum(p.shape[0] for p in first)
            return jnp.concatenate(first + second, axis=0), count

        def run(hops, gate):
            query, count = pick(hops)
            if gate is not None:
                query = after(query, gate)
            return attend(query, count, keys, values), count

        remote = list(range(1, outers))
        result, count = run(remote, gate)
        local, local_count = run([0], result)
        block = count // len(remote)
        got, got_extra = {0: local[:local_count]}, {0: local[local_count:]}
        place = count
        for k, s in enumerate(remote):
            out = result[k * block : (k + 1) * block]
            if extra_queries[s]:
                out = jnp.concatenate([out, result[place : place + block]], axis=0)
                place += block
            out = back(out, s)
            got[s], got_extra[s] = out[:block], out[block:]
        stacked = jnp.stack([got[s] for s in range(outers)])
        heads = [
            lax.dynamic_index_in_dim(stacked, (h - me) % outers, axis=0, keepdims=False)
            for h in range(outers)
        ]
        if spare:
            stacked_extra = jnp.stack([got_extra[s] for s in range(0, outers, 2)])
            for j in range(outers // 2):
                sender = 2 * j + me % 2
                heads.append(
                    lax.dynamic_index_in_dim(
                        stacked_extra, ((sender - me) % outers) // 2, axis=0, keepdims=False
                    )
                )
        mixed = jnp.concatenate(heads, axis=1)
        return (
            mixed.reshape(2, 2, block // 4, local_cols)
            .swapaxes(0, 1)
            .reshape(block, local_cols)
        )

    chunks = [range(0, outers // 2), range(outers // 2, outers)]

    def terms_of(mixed, chunk):
        return jnp.concatenate(
            [
                jnp.dot(mixed, out_full[j], preferred_element_type=jnp.float32).astype(
                    jnp.bfloat16
                )
                for j in chunk
            ],
            axis=1,
        )

    rows = tokens.shape[1]
    mixed = attended_heads(True, None)
    far, gates = [], []
    for chunk in chunks:
        terms = terms_of(mixed, chunk)
        across = swap(terms[rows:], "head")
        both = (terms[:rows].astype(jnp.float32) + across.astype(jnp.float32)).astype(
            jnp.bfloat16
        )
        far.append(swap(both, "inner"))
        gates.append(both)
    mixed = attended_heads(False, gates[-1])
    outs, start = [], 0
    for k, chunk in enumerate(chunks):
        terms = terms_of(mixed, chunk)
        near = swap(terms[rows:], "head")
        summed = (
            terms[:rows].astype(jnp.float32)
            + near.astype(jnp.float32)
            + far[k].astype(jnp.float32)
        )
        stop = start + summed.shape[1]
        outs.append((summed * gate_mod[:, start:stop]).astype(jnp.bfloat16))
        start = stop
    return jnp.concatenate(outs, axis=1)[None]


def fits(mesh):
    sizes = mesh.shape
    return (
        sizes["inner"] == 2 and sizes["head"] == 2 and sizes["clip"] <= 2
        and 4 <= sizes["outer"] <= 8 and sizes["outer"] % 2 == 0
    )


def solution(mesh):
    in_specs = (
        P("clip", ("outer", "inner", "head"), None),
        P("clip", None),
        P("clip", None),
        P("clip", None),
        P("outer", ("inner", "head")),
        P("outer", ("inner", "head")),
        P("outer", ("inner", "head")),
        P(("inner", "head"), "outer"),
        P(),
        P(),
    )
    out_specs = P("clip", ("outer", "inner", "head"), None)

    def body(*args):
        clips, outers = mesh.shape["clip"], mesh.shape["outer"]
        head_count = args[4].shape[1] // args[8].shape[0]
        placed = 2 * head_count in (2 * outers, 3 * outers)
        if fits(mesh) and placed and args[0].shape[0] == 1:
            return head_sharded(clips, outers, *args)
        return per_device(*args)

    return jax.shard_map(
        body, mesh=mesh, in_specs=in_specs, out_specs=out_specs, check_vma=False
    )
```
